32 devices in a mesh: dp: 4 (over y, x), tp: 8 (over z, core).
Axes of the slice: x: 2, y: 2, z: 4, core: 2. Of those that a mesh axis runs over, the one named last changes fastest.
Arguments:
- proj_in: bfloat16 [1, 4096, 8192], P(None, 'dp', 'tp'), may hold values from -6 to 6
- kv_grad: bfloat16 [1, 4096, 2048], P(None, ('dp', 'tp')), may hold values from -0.1796875 to 0.1796875
- normed: bfloat16 [1, 4096, 8192], P(None, ('dp', 'tp')), may hold values from -6 to 6
- norm_grad: bfloat16 [1, 4096, 8192], P(None, ('dp', 'tp')), may hold values from -0.6 to 0.6
- first_moment: float32 [1, 8192, 2048], P(None, 'tp', 'dp'), may hold values from -0.6 to 0.6
- second_moment: float32 [1, 8192, 2048], P(None, 'tp', 'dp'), may hold values from 0.002 to 0.02
Outputs:
- new_first: float32 [1, 8192, 2048], P(None, 'tp', 'dp')
- new_second: float32 [1, 8192, 2048], P(None, 'tp', 'dp')
- adam_step: float32 [1, 8192, 2048], P(None, 'tp', 'dp')
- gain_grad: float32 [1, 8192], replicated
The draws below stay inside these ranges and needn't reach their ends.
All inputs are finite; a program needn't handle non-finite values.
Results may differ from the reference program's by a relative error of at most 0.0003.
Values may be sent and summed in bfloat16 or wider, within the bound.
A program may use at most 128 MiB of HBM per device.

```python
import math
import jax
import jax.numpy as jnp
from jax import lax

D = 8192
KV = 2048
LAYERS = 1
TOK_REP = 1024
TOKENS = 4096
N_DP = 4


def draw_norm_grad(key, part):
    first_key, second_key, third_key = jax.random.split(key, 3)
    values = 0.1 * jax.random.normal(first_key, (LAYERS, TOKENS, D), jnp.float32)
    return jnp.clip(values, -0.6, 0.6).astype(jnp.bfloat16)


def strengthened(result, own_key, source, target, parts, factor):
    def block_of(position):
        return (jnp.arange(result.shape[position]) // (result.shape[position] // parts)).reshape((-1,) + (1,) * (result.ndim - 1 - position))

    one_side = jax.random.permutation(own_key, parts)[block_of(target)]
    second = (block_of(target) + parts // 2) % parts
    return jnp.where((block_of(source) == one_side) | (block_of(source) == second), factor * result, result)


def block_levels(stream_key, dims, shards, least, top_value):
    factor_of, own = 1.0, jax.random.fold_in(stream_key, 6)
    for axis_at, parts in shards:
        draws = jnp.exp(jax.random.uniform(jax.random.fold_in(own, axis_at), (parts,), jnp.float32, least / len(shards), top_value / len(shards)))
        factor_of = factor_of * jnp.repeat(draws, dims[axis_at] // parts).reshape([-1 if axis == axis_at else 1 for axis in range(len(dims))])
    return factor_of


def bell_draw(rng, extent, scale, bound, pieces=(), held_as=jnp.bfloat16):
    loudness = block_levels(rng, extent, pieces, -0.22, 0.18) if pieces else 1.0
    array = jax.random.normal(rng, extent, jnp.float32) * scale * loudness
    return jnp.minimum(jnp.maximum(array, -bound), bound).astype(held_as)


def heavy_noise(key, shape, deviation, limit, cuts, heavy, held_as=jnp.bfloat16):
    drawn = deviation * jax.random.normal(key, shape, jnp.float32)
    if cuts:
        drawn = drawn * block_levels(key, shape, cuts, -0.22, 0.18)
    return jnp.clip(strengthened(drawn, jax.random.fold_in(key, 3), *heavy), -limit, limit).astype(held_as)


def setup_inputs(seed: int = 0) -> dict:
    splits = jax.random.split(jax.random.key(seed), 7)
    return {
        "proj_in": bell_draw(splits[0], (LAYERS, TOKENS, D), 1.0, 6.0, ((1, 4), (2, 8))),
        "kv_grad": heavy_noise(splits[1], (LAYERS, TOKENS, KV), 0.03, 0.1796875, ((1, 32),), (1, 2, 32, 2.75)),
        "normed": bell_draw(splits[2], (LAYERS, TOKENS, D), 1.0, 6.0, ((1, 32),)),
        "norm_grad": draw_norm_grad(jax.random.fold_in(splits[6], 71), 0),
        "first_moment": bell_draw(splits[4], (LAYERS, D, KV), 0.1, 0.6, ((1, 8), (2, 4)), jnp.float32),
        "second_moment": jnp.clip(jnp.exp(math.log(0.02) - 2.30258502 * jax.random.uniform(splits[5], (LAYERS, D, KV), jnp.float32) ** block_levels(splits[5], (LAYERS, D, KV), ((1, 8), (2, 4)), -0.2, 0.2)), 0.002, 0.02),
    }


beta_one = 0.9
beta_two = 0.95
correct_one = 0.19
correct_two = 0.0975
epsilon = 1e-08

def reference(proj_in, kv_grad, normed, norm_grad, first_moment, second_moment):
    firsts = []
    seconds = []
    updates = []
    for layer_id in range(LAYERS):
        running = jnp.zeros((D, KV), jnp.float32)
        for replica in range(N_DP):
            inputs = proj_in[layer_id, replica * TOK_REP:(replica + 1) * TOK_REP]
            grad_rows = kv_grad[layer_id, replica * TOK_REP:(replica + 1) * TOK_REP]
            product = lax.dot_general(inputs, grad_rows, (((0,), (0,)), ((), ())), preferred_element_type=jnp.float32)
            running = running + product
        mean_grad = running / N_DP
        new_first = beta_one * first_moment[layer_id] + (1.0 - beta_one) * mean_grad
        new_second = beta_two * second_moment[layer_id] + (1.0 - beta_two) * mean_grad * mean_grad
        update = new_first / correct_one / (jnp.sqrt(new_second / correct_two) + epsilon)
        firsts.append(new_first)
        seconds.append(new_second)
        updates.append(update)
    gain_grad = lax.optimization_barrier(jnp.sum(norm_grad.astype(jnp.float32) * normed.astype(jnp.float32), axis=1)) / N_DP
    return (jnp.stack(firsts), jnp.stack(seconds), jnp.stack(updates), gain_grad)
```

```python
import functools

import jax
import jax.numpy as jnp
from jax import lax
from jax.experimental import pallas as pl
from jax.experimental.pallas import tpu as pltpu
from jax.sharding import PartitionSpec as P

beta_one = 0.9
beta_two = 0.95
correct_one = 0.19
correct_two = 0.0975
epsilon = 1e-08
PIECES = 4


def adam_update(mean_grad, first_old, second_old):
    new_first = beta_one * first_old + (1.0 - beta_one) * mean_grad
    new_second = beta_two * second_old + (1.0 - beta_two) * mean_grad * mean_grad
    update = new_first / correct_one / (jnp.sqrt(new_second / correct_two) + epsilon)
    return (new_first, new_second, update)


def kernel(
    n_dp, n_tp, x_hbm, g_hbm, a_hbm, b_hbm, sum_ref, gain_ref,
    xs, kv, a_buf, b_buf, gain_tp, gain_dp,
    local_sem, x_send, x_recv, a2a_send, a2a_recv,
    up_send, up_recv, down_send, down_recv, pair_send, pair_recv,
    gt_send, gt_recv, gd_send, gd_recv,
):
    dp = lax.axis_index("dp")
    tp = lax.axis_index("tp")
    z = tp // 2
    core = tp % 2
    n_z = n_tp // 2
    rows = g_hbm.shape[0]
    cols = kv.shape[2]
    tokens = x_hbm.shape[0]
    piece = tokens // PIECES

    def dp_peer(o):
        return jnp.bitwise_xor(dp, o)

    def tp_peer(o):
        return lax.rem(tp + o, n_tp)

    locals_ = [
        pltpu.make_async_copy(a_hbm, a_buf, local_sem.at[0]),
        pltpu.make_async_copy(b_hbm, b_buf, local_sem.at[1]),
        pltpu.make_async_copy(
            g_hbm.at[:, pl.ds(pl.multiple_of(dp * cols, cols), cols)],
            kv.at[dp, pl.ds(pl.multiple_of(tp * rows, rows), rows), :],
            local_sem.at[2],
        ),
        pltpu.make_async_copy(x_hbm, xs.at[dp], local_sem.at[3]),
    ]
    for copy in locals_:
        copy.start()

    barrier = pltpu.get_barrier_semaphore()
    for o in range(1, n_dp):
        pl.semaphore_signal(barrier, inc=1, device_id={"dp": dp_peer(o)}, device_id_type=pl.DeviceIdType.MESH)
    for o in range(1, n_tp):
        pl.semaphore_signal(barrier, inc=1, device_id={"tp": tp_peer(o)}, device_id_type=pl.DeviceIdType.MESH)
    pl.semaphore_wait(barrier, n_dp - 1 + n_tp - 1)

    sent = []

    def remote(src, dst, send, recv, where):
        return pltpu.make_async_remote_copy(
            src_ref=src, dst_ref=dst, send_sem=send, recv_sem=recv,
            device_id=where, device_id_type=pl.DeviceIdType.MESH,
        )

    my_rows = pl.ds(pl.multiple_of(tp * rows, rows), rows)
    a2a = []
    for o in range(1, n_dp):
        peer = dp_peer(o)
        copy = remote(
            g_hbm.at[:, pl.ds(pl.multiple_of(peer * cols, cols), cols)],
            kv.at[dp, my_rows, :], a2a_send.at[o], a2a_recv.at[o], {"dp": peer},
        )
        copy.start()
        a2a.append(copy)
        sent.append(copy)

    def x_copy(src, origin, c, o_recv, o_to, send):
        part = pl.ds(c * piece, piece)
        return remote(
            src.at[part, :], xs.at[origin, part, :], send, x_recv.at[o_recv, c],
            {"dp": dp_peer(o_to)},
        )

    square = n_dp == 4
    orders = {o: list(range(PIECES)) for o in range(1, n_dp)}
    half = PIECES // 2
    if square:
        orders[2] = list(range(half, PIECES)) + list(range(half))
        orders[3] = []

    def send_own(i):
        for o in range(1, n_dp):
            if i < len(orders[o]):
                c = orders[o][i]
                copy = x_copy(x_hbm, dp, c, o, o, x_send.at[o, c])
                copy.start()
                sent.append(copy)

    def got(o, c):
        x_copy(xs.at[dp_peer(o)], dp_peer(o), c, o, o, x_send.at[o, c]).wait_recv()

    def forward(i):
        for o, o_to in ((1, 2), (2, 1)):
            c = orders[o][i]
            got(o, c)
            copy = x_copy(xs.at[dp_peer(o)], dp_peer(o), c, 3, o_to, x_send.at[3, c])
            copy.start()
            sent.append(copy)

    send_own(0)
    send_own(1)

    locals_[0].wait()
    locals_[1].wait()
    wide = gain_tp.shape[2]
    lines = gain_tp.shape[1]
    for j in range(lines):
        s = pl.ds(j * wide, wide)
        products = a_buf[:, s].astype(jnp.float32) * b_buf[:, s].astype(jnp.float32)
        gain_tp[tp, pl.ds(j, 1), :] = jnp.sum(products, axis=0, keepdims=True)
    tp_copies = []
    for o in range(1, n_tp):
        copy = remote(gain_tp.at[tp], gain_tp.at[tp], gt_send.at[o], gt_recv.at[o], {"tp": tp_peer(o)})
        copy.start()
        sent.append(copy)
        tp_copies.append(copy)

    def block(b, c):
        return kv.at[:, pl.ds(pl.multiple_of((2 * b + c) * rows, rows), rows), :]

    other = 2 * z + 1 - core

    def to_pair(b):
        return remote(block(b, core), block(b, core), pair_send.at[b], pair_recv.at[b], {"tp": other})

    def up(s):
        b = z - s + 1
        return remote(block(b, core), block(b, core), up_send.at[s], up_recv.at[s], {"tp": tp + 2})

    def down(s):
        b = z + s - 1
        return remote(block(b, core), block(b, core), down_send.at[s], down_recv.at[s], {"tp": tp - 2})

    def up_got(s):
        b = z - s
        return remote(block(b, core), block(b, core), up_send.at[s], up_recv.at[s], {"tp": other})

    def down_got(s):
        b = z + s
        return remote(block(b, core), block(b, core), down_send.at[s], down_recv.at[s], {"tp": other})

    locals_[2].wait()
    for o in range(1, n_dp):
        a2a[o - 1].wait_recv()

    for s in range(1, n_z + 1):
        if s > 1:
            @pl.when(z - s + 1 >= 0)
            def _():
                up_got(s - 1).wait_recv()

        if s < n_z:
            @pl.when((z - s + 1 >= 0) & (z + 1 < n_z))
            def _():
                up(s).start()

        if s > 1:
            @pl.when(z + s - 1 < n_z)
            def _():
                down_got(s - 1).wait_recv()

        if s < n_z:
            @pl.when((z + s - 1 < n_z) & (z - 1 >= 0))
            def _():
                down(s).start()

        if s == 1:
            to_pair(z).start()
        else:
            @pl.when(z - s + 1 >= 0)
            def _():
                to_pair(z - s + 1).start()

            @pl.when(z + s - 1 < n_z)
            def _():
                to_pair(z + s - 1).start()

        if s == 1:
            for copy in tp_copies:
                copy.wait_recv()
            gain_dp[dp, :, :] = jnp.sum(gain_tp[...], axis=0)
            for o in range(1, n_dp):
                copy = remote(gain_dp.at[dp], gain_dp.at[dp], gd_send.at[o], gd_recv.at[o], {"dp": dp_peer(o)})
                copy.start()
                sent.append(copy)
            for i in range(2, PIECES):
                send_own(i)
        if square and 2 <= s < 2 + half:
            forward(s - 2)
    if square:
        for i in range(max(n_z - 1, 0), half):
            forward(i)

    for b in range(n_z):
        remote(block(b, 1 - core), block(b, 1 - core), pair_send.at[b], pair_recv.at[b], {"tp": other}).wait_recv()

    width = min(256, sum_ref.shape[0])

    def multiply(origin, start, size, first=False):
        @pl.loop(0, sum_ref.shape[0] // width)
        def _(f):
            at = pl.ds(pl.multiple_of(f * width, width), width)
            part = lax.dot_general(
                xs[origin, pl.ds(start, size), at], kv[origin, pl.ds(start, size), :],
                (((0,), (0,)), ((), ())), preferred_element_type=jnp.float32,
            )
            if first:
                sum_ref[at, :] = part
            else:
                sum_ref[at, :] += part

    locals_[3].wait()
    multiply(dp, 0, tokens, True)
    for o in range(1, n_dp):
        if square and o == 3:
            continue
        for c in orders[o]:
            if not (square and c in orders[o][:half]):
                got(o, c)
        multiply(dp_peer(o), 0, tokens)

    for o in range(1, n_dp):
        remote(gain_dp.at[dp_peer(o)], gain_dp.at[dp_peer(o)], gd_send.at[o], gd_recv.at[o], {"dp": dp_peer(o)}).wait_recv()
    gain_ref[...] = jnp.sum(gain_dp[...], axis=0) / n_dp

    if square:
        for i in range(half):
            for o in (1, 2):
                c = orders[o][i]
                got(3, c)
                multiply(dp_peer(3), c * piece, piece)

    for copy in sent:
        copy.wait_send()
    for s in range(1, n_z):
        @pl.when((z - s + 1 >= 0) & (z + 1 < n_z))
        def _():
            up(s).wait_send()

        @pl.when((z + s - 1 < n_z) & (z - 1 >= 0))
        def _():
            down(s).wait_send()
    for b in range(n_z):
        to_pair(b).wait_send()


def shards(n_dp, n_tp, proj_in, kv_grad, normed, norm_grad, first_moment, second_moment):
    layers, tokens, features = proj_in.shape
    rows, width = kv_grad.shape[1:]
    model = normed.shape[2]
    cols = width // n_dp
    lines = 8
    dma = pltpu.SemaphoreType.DMA
    n_z = n_tp // 2
    firsts, seconds, updates, gains = [], [], [], []
    for layer in range(layers):
        total, gain = pl.pallas_call(
            functools.partial(kernel, n_dp, n_tp),
            out_shape=(
                jax.ShapeDtypeStruct((features, cols), jnp.float32),
                jax.ShapeDtypeStruct((lines, model // lines), jnp.float32),
            ),
            in_specs=[pl.BlockSpec(memory_space=pl.ANY)] * 4,
            out_specs=(pl.BlockSpec(memory_space=pltpu.VMEM), pl.BlockSpec(memory_space=pltpu.VMEM)),
            scratch_shapes=[
                pltpu.VMEM((n_dp, tokens, features), jnp.bfloat16),
                pltpu.VMEM((n_dp, n_tp * rows, cols), jnp.bfloat16),
                pltpu.VMEM((rows, model), jnp.bfloat16),
                pltpu.VMEM((rows, model), jnp.bfloat16),
                pltpu.VMEM((n_tp, lines, model // lines), jnp.float32),
                pltpu.VMEM((n_dp, lines, model // lines), jnp.float32),
                dma((4,)),
                dma((n_dp, PIECES)), dma((n_dp, PIECES)),
                dma((n_dp,)), dma((n_dp,)),
                dma((n_z,)), dma((n_z,)), dma((n_z,)), dma((n_z,)),
                dma((n_z,)), dma((n_z,)),
                dma((n_tp,)), dma((n_tp,)), dma((n_dp,)), dma((n_dp,)),
            ],
            compiler_params=pltpu.CompilerParams(
                collective_id=layer, has_side_effects=True, vmem_limit_bytes=60 * 1024 * 1024,
            ),
        )(proj_in[layer], kv_grad[layer], normed[layer], norm_grad[layer])
        new_first, new_second, update = adam_update(total / n_dp, first_moment[layer], second_moment[layer])
        firsts.append(new_first)
        seconds.append(new_second)
        updates.append(update)
        gains.append(gain.reshape(model))
    return (jnp.stack(firsts), jnp.stack(seconds), jnp.stack(updates), jnp.stack(gains))


def solution(mesh):
    return jax.shard_map(
        functools.partial(shards, mesh.shape["dp"], mesh.shape["tp"]),
        mesh=mesh,
        in_specs=(
            P(None, "dp", "tp"),
            P(None, ("dp", "tp"), None),
            P(None, ("dp", "tp"), None),
            P(None, ("dp", "tp"), None),
            P(None, "tp", "dp"),
            P(None, "tp", "dp"),
        ),
        out_specs=(P(None, "tp", "dp"), P(None, "tp", "dp"), P(None, "tp", "dp"), P()),
        check_vma=False,
    )
```

```python
import functools

import jax
import jax.numpy as jnp
from jax import lax
from jax.experimental import pallas as pl
from jax.experimental.pallas import tpu as pltpu
from jax.sharding import PartitionSpec as P

beta_one = 0.9
beta_two = 0.95
correct_one = 0.19
correct_two = 0.0975
epsilon = 1e-08
PIECES = 4
HEADS = 6


def adam_update(mean_grad, first_old, second_old):
    new_first = beta_one * first_old + (1.0 - beta_one) * mean_grad
    new_second = beta_two * second_old + (1.0 - beta_two) * mean_grad * mean_grad
    update = new_first / correct_one / (jnp.sqrt(new_second / correct_two) + epsilon)
    return (new_first, new_second, update)


def kernel(
    n_dp, n_tp, x_hbm, g_hbm, a_hbm, b_hbm, sum_ref, gain_ref,
    xs, kv, a_buf, b_buf, gain_tp, gain_dp,
    local_sem, x_send, x_recv, a2a_send, a2a_recv,
    up_send, up_recv, down_send, down_recv, pair_send, pair_recv,
    gt_send, gt_recv, gd_send, gd_recv,
):
    dp = lax.axis_index("dp")
    tp = lax.axis_index("tp")
    z = tp // 2
    core = tp % 2
    n_z = n_tp // 2
    rows = g_hbm.shape[0]
    cols = kv.shape[2]
    tokens = x_hbm.shape[0]
    piece = tokens // PIECES

    def dp_peer(o):
        return jnp.bitwise_xor(dp, o)

    def tp_peer(o):
        return lax.rem(tp + o, n_tp)

    locals_ = [
        pltpu.make_async_copy(a_hbm, a_buf, local_sem.at[0]),
        pltpu.make_async_copy(b_hbm, b_buf, local_sem.at[1]),
        pltpu.make_async_copy(
            g_hbm.at[:, pl.ds(pl.multiple_of(dp * cols, cols), cols)],
            kv.at[dp, pl.ds(pl.multiple_of(tp * rows, rows), rows), :],
            local_sem.at[2],
        ),
        pltpu.make_async_copy(x_hbm, xs.at[dp], local_sem.at[3]),
    ]
    for copy in locals_:
        copy.start()

    barrier = pltpu.get_barrier_semaphore()
    for o in range(1, n_dp):
        pl.semaphore_signal(barrier, inc=1, device_id={"dp": dp_peer(o)}, device_id_type=pl.DeviceIdType.MESH)
    for o in range(1, n_tp):
        pl.semaphore_signal(barrier, inc=1, device_id={"tp": tp_peer(o)}, device_id_type=pl.DeviceIdType.MESH)
    pl.semaphore_wait(barrier, n_dp - 1 + n_tp - 1)

    sent = []

    def remote(src, dst, send, recv, where):
        return pltpu.make_async_remote_copy(
            src_ref=src, dst_ref=dst, send_sem=send, recv_sem=recv,
            device_id=where, device_id_type=pl.DeviceIdType.MESH,
        )

    my_rows = pl.ds(pl.multiple_of(tp * rows, rows), rows)
    a2a = []
    for o in range(1, n_dp):
        peer = dp_peer(o)
        copy = remote(
            g_hbm.at[:, pl.ds(pl.multiple_of(peer * cols, cols), cols)],
            kv.at[dp, my_rows, :], a2a_send.at[o], a2a_recv.at[o], {"dp": peer},
        )
        copy.start()
        a2a.append(copy)
        sent.append(copy)

    def x_copy(src, origin, c, o_recv, o_to, send):
        part = pl.ds(c * piece, piece)
        return remote(
            src.at[part, :], xs.at[origin, part, :], send, x_recv.at[o_recv, c],
            {"dp": dp_peer(o_to)},
        )

    square = n_dp == 4
    orders = {o: list(range(PIECES)) for o in range(1, n_dp)}
    half = PIECES // 2
    if square:
        orders[2] = list(range(half, PIECES)) + list(range(half))
        orders[3] = []

    def send_own(i):
        for o in range(1, n_dp):
            if i < len(orders[o]):
                c = orders[o][i]
                copy = x_copy(x_hbm, dp, c, o, o, x_send.at[o, c])
                copy.start()
                sent.append(copy)

    def got(o, c):
        x_copy(xs.at[dp_peer(o)], dp_peer(o), c, o, o, x_send.at[o, c]).wait_recv()

    def forward(i):
        for o, o_to in ((1, 2), (2, 1)):
            c = orders[o][i]
            got(o, c)
            copy = x_copy(xs.at[dp_peer(o)], dp_peer(o), c, 3, o_to, x_send.at[3, c])
            copy.start()
            sent.append(copy)

    send_own(0)
    send_own(1)

    locals_[0].wait()
    locals_[1].wait()
    wide = gain_tp.shape[2]
    lines = gain_tp.shape[1]
    for j in range(lines):
        s = pl.ds(j * wide, wide)
        products = a_buf[:, s].astype(jnp.float32) * b_buf[:, s].astype(jnp.float32)
        gain_tp[tp, pl.ds(j, 1), :] = jnp.sum(products, axis=0, keepdims=True)
    tp_copies = []
    for o in range(1, n_tp):
        copy = remote(gain_tp.at[tp], gain_tp.at[tp], gt_send.at[o], gt_recv.at[o], {"tp": tp_peer(o)})
        copy.start()
        sent.append(copy)
        tp_copies.append(copy)

    def block(b, c):
        return kv.at[:, pl.ds(pl.multiple_of((2 * b + c) * rows, rows), rows), :]

    other = 2 * z + 1 - core

    def to_pair(b):
        return remote(block(b, core), block(b, core), pair_send.at[b], pair_recv.at[b], {"tp": other})

    def up(s):
        b = z - s + 1
        return remote(block(b, core), block(b, core), up_send.at[s], up_recv.at[s], {"tp": tp + 2})

    def down(s):
        b = z + s - 1
        return remote(block(b, core), block(b, core), down_send.at[s], down_recv.at[s], {"tp": tp - 2})

    def up_got(s):
        b = z - s
        return remote(block(b, core), block(b, core), up_send.at[s], up_recv.at[s], {"tp": other})

    def down_got(s):
        b = z + s
        return remote(block(b, core), block(b, core), down_send.at[s], down_recv.at[s], {"tp": other})

    locals_[2].wait()
    for o in range(1, n_dp):
        a2a[o - 1].wait_recv()

    for s in range(1, n_z + 1):
        if s > 1:
            @pl.when(z - s + 1 >= 0)
            def _():
                up_got(s - 1).wait_recv()

        if s < n_z:
            @pl.when((z - s + 1 >= 0) & (z + 1 < n_z))
            def _():
                up(s).start()

        if s > 1:
            @pl.when(z + s - 1 < n_z)
            def _():
                down_got(s - 1).wait_recv()

        if s < n_z:
            @pl.when((z + s - 1 < n_z) & (z - 1 >= 0))
            def _():
                down(s).start()

        if s == 1:
            to_pair(z).start()
        else:
            @pl.when(z - s + 1 >= 0)
            def _():
                to_pair(z - s + 1).start()

            @pl.when(z + s - 1 < n_z)
            def _():
                to_pair(z + s - 1).start()

        if s == 1:
            for copy in tp_copies:
                copy.wait_recv()
            gain_dp[dp, :, :] = jnp.sum(gain_tp[...], axis=0)
            for o in range(1, n_dp):
                copy = remote(gain_dp.at[dp], gain_dp.at[dp], gd_send.at[o], gd_recv.at[o], {"dp": dp_peer(o)})
                copy.start()
                sent.append(copy)
            for i in range(2, PIECES):
                send_own(i)
        if square and 2 <= s < 2 + half:
            forward(s - 2)
    if square:
        for i in range(max(n_z - 1, 0), half):
            forward(i)

    for b in range(n_z):
        remote(block(b, 1 - core), block(b, 1 - core), pair_send.at[b], pair_recv.at[b], {"tp": other}).wait_recv()

    width = min(256, sum_ref.shape[0])

    def multiply(origin, start, size, first=False):
        @pl.loop(0, sum_ref.shape[0] // width)
        def _(f):
            at = pl.ds(pl.multiple_of(f * width, width), width)
            part = lax.dot_general(
                xs[origin, pl.ds(start, size), at], kv[origin, pl.ds(start, size), :],
                (((0,), (0,)), ((), ())), preferred_element_type=jnp.float32,
            )
            if first:
                sum_ref[at, :] = part
            else:
                sum_ref[at, :] += part

    locals_[3].wait()
    multiply(dp, 0, tokens, True)
    for o in range(1, n_dp):
        if square and o == 3:
            continue
        for c in orders[o]:
            if not (square and c in orders[o][:half]):
                got(o, c)
        multiply(dp_peer(o), 0, tokens)

    for o in range(1, n_dp):
        remote(gain_dp.at[dp_peer(o)], gain_dp.at[dp_peer(o)], gd_send.at[o], gd_recv.at[o], {"dp": dp_peer(o)}).wait_recv()
    gain_ref[...] = jnp.sum(gain_dp[...], axis=0) / n_dp

    if square:
        for i in range(half):
            for o in (1, 2):
                c = orders[o][i]
                got(3, c)
                multiply(dp_peer(3), c * piece, piece)

    for copy in sent:
        copy.wait_send()
    for s in range(1, n_z):
        @pl.when((z - s + 1 >= 0) & (z + 1 < n_z))
        def _():
            up(s).wait_send()

        @pl.when((z + s - 1 < n_z) & (z - 1 >= 0))
        def _():
            down(s).wait_send()
    for b in range(n_z):
        to_pair(b).wait_send()


def square_kernel(
    n_tp, x_hbm, g_hbm, a_hbm, b_hbm, sum_ref, gain_ref,
    xs, xb, kv, kvp, part, arrived, a_buf, b_buf, gain_pair, gain_z, gain_dp,
    local_sem, head_send, head_recv, whole_send, whole_recv, fwd_send, fwd_recv,
    part_send, part_recv, a2a_send, a2a_recv,
    up_send, up_recv, down_send, down_recv, pair_send, pair_recv,
    gp_send, gp_recv, gz_send, gz_recv, gd_send, gd_recv,
):
    n_dp = 4
    dp = lax.axis_index("dp")
    tp = lax.axis_index("tp")
    z = tp // 2
    core = tp % 2
    n_z = n_tp // 2
    rows = g_hbm.shape[0]
    cols = kv.shape[2]
    tokens, features = x_hbm.shape
    head = part.shape[0]
    tail = features - head
    chunk = head // HEADS
    half = tokens // 2
    other = 2 * z + 1 - core
    sent = []

    def dp_peer(o):
        return jnp.bitwise_xor(dp, o)

    def remote(src, dst, send, recv, where):
        return pltpu.make_async_remote_copy(
            src_ref=src, dst_ref=dst, send_sem=send, recv_sem=recv,
            device_id=where, device_id_type=pl.DeviceIdType.MESH,
        )

    def go(copy):
        copy.start()
        sent.append(copy)

    my_rows = pl.ds(pl.multiple_of(tp * rows, rows), rows)

    def g_cols(d):
        return g_hbm.at[:, pl.ds(pl.multiple_of(d * cols, cols), cols)]

    locals_ = [
        pltpu.make_async_copy(g_cols(dp_peer(2)), kvp.at[0, my_rows, :], local_sem.at[0]),
        pltpu.make_async_copy(a_hbm, a_buf, local_sem.at[1]),
        pltpu.make_async_copy(b_hbm, b_buf, local_sem.at[2]),
        pltpu.make_async_copy(g_cols(dp), kv.at[dp, my_rows, :], local_sem.at[3]),
        pltpu.make_async_copy(x_hbm, xs.at[0], local_sem.at[4]),
    ]
    for copy in locals_:
        copy.start()

    barrier = pltpu.get_barrier_semaphore()
    for o in range(1, n_dp):
        pl.semaphore_signal(barrier, inc=1, device_id={"dp": dp_peer(o)}, device_id_type=pl.DeviceIdType.MESH)
    for o in range(1, n_tp):
        pl.semaphore_signal(barrier, inc=1, device_id={"tp": lax.rem(tp + o, n_tp)}, device_id_type=pl.DeviceIdType.MESH)
    pl.semaphore_wait(barrier, n_dp - 1 + n_tp - 1)

    pair_base = dp // 2 * 2
    groups = [
        kvp.at[pl.ds(0, 1)],
        kvp.at[pl.ds(1, 1)],
        kv.at[pl.ds(pair_base, 2)],
        kv.at[pl.ds(2 - pair_base, 2)],
    ]

    def block(g, b, c):
        return groups[g].at[:, pl.ds(pl.multiple_of((2 * b + c) * rows, rows), rows), :]

    def to_pair(g, b):
        return remote(block(g, b, core), block(g, b, core), pair_send.at[g, b], pair_recv.at[g, b], {"tp": other})

    def from_pair(g, b):
        return remote(block(g, b, 1 - core), block(g, b, 1 - core), pair_send.at[g, b], pair_recv.at[g, b], {"tp": other})

    def up(g, s):
        b = z - s + 1
        return remote(block(g, b, core), block(g, b, core), up_send.at[g, s], up_recv.at[g, s], {"tp": tp + 2})

    def down(g, s):
        b = z + s - 1
        return remote(block(g, b, core), block(g, b, core), down_send.at[g, s], down_recv.at[g, s], {"tp": tp - 2})

    def up_got(g, s):
        b = z - s
        return remote(block(g, b, core), block(g, b, core), up_send.at[g, s], up_recv.at[g, s], {"tp": other})

    def down_got(g, s):
        b = z + s
        return remote(block(g, b, core), block(g, b, core), down_send.at[g, s], down_recv.at[g, s], {"tp": other})

    def chain(g, s):
        if s > 1:
            @pl.when(z - s + 1 >= 0)
            def _():
                up_got(g, s - 1).wait_recv()

        if s < n_z:
            @pl.when((z - s + 1 >= 0) & (z + 1 < n_z))
            def _():
                up(g, s).start()

        if s > 1:
            @pl.when(z + s - 1 < n_z)
            def _():
                down_got(g, s - 1).wait_recv()

        if s < n_z:
            @pl.when((z + s - 1 < n_z) & (z - 1 >= 0))
            def _():
                down(g, s).start()

        if s == 1:
            to_pair(g, z).start()
        else:
            @pl.when(z - s + 1 >= 0)
            def _():
                to_pair(g, z - s + 1).start()

            @pl.when(z + s - 1 < n_z)
            def _():
                to_pair(g, z + s - 1).start()

    def complete(g):
        for b in range(n_z):
            from_pair(g, b).wait_recv()

    swap = remote(g_cols(dp_peer(3)), kvp.at[1, my_rows, :], a2a_send.at[0], a2a_recv.at[0], {"dp": dp_peer(1)})
    go(swap)
    locals_[0].wait()
    chain(0, 1)

    def a2a(o, origin):
        return remote(g_cols(dp_peer(o)), kv.at[origin, my_rows, :], a2a_send.at[o], a2a_recv.at[o], {"dp": dp_peer(o)})

    for o in range(1, n_dp):
        go(a2a(o, dp))

    tail_at = pl.ds(head, tail)

    def head_copy(k):
        at = pl.ds(k * chunk, chunk)
        return remote(x_hbm.at[:, at], xs.at[1, :, at], head_send.at[k], head_recv.at[k], {"dp": dp_peer(1)})

    def tail_copy(o, h):
        at = pl.ds(h * half, half)
        dst = xs.at[1, at, tail_at] if o == 1 else xb.at[0, at, :]
        return remote(x_hbm.at[at, tail_at], dst, whole_send.at[o, h], whole_recv.at[o, h], {"dp": dp_peer(o)})

    def forward(h):
        at = pl.ds(h * half, half)
        src = xs.at[1, at, tail_at] if h == 0 else xb.at[0, at, :]
        return remote(src, xb.at[1, at, :], fwd_send.at[h], fwd_recv.at[h], {"dp": dp_peer(2 - h)})

    early = HEADS // 2
    for k in range(early):
        go(head_copy(k))
    go(tail_copy(2, 1))
    go(tail_copy(2, 0))

    locals_[1].wait()
    locals_[2].wait()
    wide = gain_pair.shape[2]

    def gain_lines(lo, hi):
        for j in range(lo, hi):
            at = pl.ds(j * wide, wide)
            products = a_buf[:, at].astype(jnp.float32) * b_buf[:, at].astype(jnp.float32)
            gain_pair[core, pl.ds(j, 1), :] = jnp.sum(products, axis=0, keepdims=True)

    lines = gain_pair.shape[1]
    gain_lines(0, lines)
    swap.wait_recv()
    chain(1, 1)
    gain_core = remote(gain_pair.at[core], gain_pair.at[core], gp_send.at[0], gp_recv.at[0], {"tp": other})
    go(gain_core)
    for s in range(2, n_z + 1):
        chain(0, s)
        chain(1, s)

    gain_core.wait_recv()
    gain_z[z, :, :] = jnp.sum(gain_pair[...], axis=0)
    for o in range(1, n_z):
        go(remote(gain_z.at[z], gain_z.at[z], gz_send.at[o], gz_recv.at[o], {"tp": lax.rem(tp + 2 * o, n_tp)}))

    for o in (1, 2, 3):
        a2a(o, dp_peer(o)).wait_recv()
    locals_[3].wait()
    chain(2, 1)
    locals_[4].wait()
    for k in range(early, HEADS):
        go(head_copy(k))
    complete(0)
    complete(1)

    def dot(x, w):
        return lax.dot_general(x, w, (((0,), (0,)), ((), ())), preferred_element_type=jnp.float32)

    def part_copy(k):
        at = pl.ds(k * chunk, chunk)
        return remote(part.at[at, :], arrived.at[at, :], part_send.at[k], part_recv.at[k], {"dp": dp_peer(2)})

    for k in range(HEADS):
        at = pl.ds(k * chunk, chunk)
        head_copy(k).wait_recv()
        part[at, :] = dot(xs[0, :, at], kvp[0]) + dot(xs[1, :, at], kvp[1])
        go(part_copy(k))
        if k == 1:
            for o in range(1, n_z):
                copy = remote(
                    gain_z.at[lax.rem(z + o, n_z)], gain_z.at[lax.rem(z + o, n_z)],
                    gz_send.at[n_z - o], gz_recv.at[n_z - o], {"tp": other},
                )
                copy.wait_recv()
            gain_dp[dp, :, :] = jnp.sum(gain_z[...], axis=0)
            for o in range(1, n_dp):
                go(remote(gain_dp.at[dp], gain_dp.at[dp], gd_send.at[o], gd_recv.at[o], {"dp": dp_peer(o)}))
            chain(2, 2)
        if k == 2:
            go(tail_copy(1, 0))
            go(tail_copy(1, 1))
        if k == 3:
            tail_copy(2, 1).wait_recv()
            go(forward(1))
            chain(2, 3)
            chain(3, 1)
        if k == HEADS - 2:
            for s in range(4, n_z + 1):
                chain(2, s)
    complete(2)
    chain(3, 2)

    def head_sum(k):
        at = pl.ds(k * chunk, chunk)
        sum_ref[at, :] = dot(xs[0, :, at], kv[dp]) + dot(xs[1, :, at], kv[dp_peer(1)])

    for k in range(HEADS // 2):
        head_sum(k)
    tail_copy(1, 0).wait_recv()
    go(forward(0))
    chain(3, 3)
    for k in range(HEADS // 2, HEADS):
        head_sum(k)
    tail_copy(1, 1).wait_recv()
    sum_ref[tail_at, :] = dot(xs[0, :, tail_at], kv[dp]) + dot(xs[1, :, tail_at], kv[dp_peer(1)])
    for s in range(4, n_z + 1):
        chain(3, s)
    for o in range(1, n_dp):
        remote(gain_dp.at[dp_peer(o)], gain_dp.at[dp_peer(o)], gd_send.at[o], gd_recv.at[o], {"dp": dp_peer(o)}).wait_recv()
    gain_ref[...] = jnp.sum(gain_dp[...], axis=0) / n_dp
    for k in range(HEADS):
        at = pl.ds(k * chunk, chunk)
        part_copy(k).wait_recv()
        sum_ref[at, :] += arrived[at, :]
    complete(3)
    tail_copy(2, 0).wait_recv()
    sum_ref[tail_at, :] += dot(xb[0], kv[dp_peer(2)])
    for h in (1, 0):
        forward(h).wait_recv()
        at = pl.ds(h * half, half)
        sum_ref[tail_at, :] += dot(xb[1, at, :], kv[dp_peer(3), at, :])

    for copy in sent:
        copy.wait_send()
    for g in range(len(groups)):
        for s in range(1, n_z):
            @pl.when((z - s + 1 >= 0) & (z + 1 < n_z))
            def _():
                up(g, s).wait_send()

            @pl.when((z + s - 1 < n_z) & (z - 1 >= 0))
            def _():
                down(g, s).wait_send()
        for b in range(n_z):
            to_pair(g, b).wait_send()


def square_call(layer, n_tp, x, g, a, b):
    tokens, features = x.shape
    rows, width = g.shape
    model = a.shape[1]
    n_dp = 4
    cols = width // n_dp
    lines = 8
    n_z = n_tp // 2
    head = features // (HEADS + 2) * HEADS
    dma = pltpu.SemaphoreType.DMA
    bf16, f32 = jnp.bfloat16, jnp.float32
    buffers = [
        ((2, tokens, features), bf16), ((2, tokens, features - head), bf16),
        ((n_dp, tokens, cols), bf16), ((2, tokens, cols), bf16),
        ((head, cols), f32), ((head, cols), f32),
        ((rows, model), bf16), ((rows, model), bf16),
        ((2, lines, model // lines), f32), ((n_z, lines, model // lines), f32), ((n_dp, lines, model // lines), f32),
    ]
    return pl.pallas_call(
        functools.partial(square_kernel, n_tp),
        out_shape=(
            jax.ShapeDtypeStruct((features, cols), f32),
            jax.ShapeDtypeStruct((lines, model // lines), f32),
        ),
        in_specs=[pl.BlockSpec(memory_space=pl.ANY)] * 4,
        out_specs=(pl.BlockSpec(memory_space=pltpu.VMEM), pl.BlockSpec(memory_space=pltpu.VMEM)),
        scratch_shapes=[pltpu.VMEM(shape, dtype) for shape, dtype in buffers] + [
            dma((5,)), dma((HEADS,)), dma((HEADS,)), dma((3, 2)), dma((3, 2)), dma((2,)), dma((2,)),
            dma((HEADS,)), dma((HEADS,)), dma((n_dp,)), dma((n_dp,)),
        ] + [dma((4, n_z))] * 6 + [
            dma((1,)), dma((1,)), dma((n_z,)), dma((n_z,)), dma((n_dp,)), dma((n_dp,)),
        ],
        compiler_params=pltpu.CompilerParams(
            collective_id=layer, has_side_effects=True, vmem_limit_bytes=60 * 1024 * 1024,
        ),
    )(x, g, a, b)


def shards(n_dp, n_tp, proj_in, kv_grad, normed, norm_grad, first_moment, second_moment):
    layers, tokens, features = proj_in.shape
    rows, width = kv_grad.shape[1:]
    model = normed.shape[2]
    cols = width // n_dp
    lines = 8
    dma = pltpu.SemaphoreType.DMA
    n_z = n_tp // 2
    firsts, seconds, updates, gains = [], [], [], []
    for layer in range(layers):
        if n_dp == 4 and features % (128 * (HEADS + 2)) == 0 and n_tp >= 6:
            total, gain = square_call(layer, n_tp, proj_in[layer], kv_grad[layer], normed[layer], norm_grad[layer])
        else:
            total, gain = pl.pallas_call(
                functools.partial(kernel, n_dp, n_tp),
                out_shape=(
                    jax.ShapeDtypeStruct((features, cols), jnp.float32),
                    jax.ShapeDtypeStruct((lines, model // lines), jnp.float32),
                ),
                in_specs=[pl.BlockSpec(memory_space=pl.ANY)] * 4,
                out_specs=(pl.BlockSpec(memory_space=pltpu.VMEM), pl.BlockSpec(memory_space=pltpu.VMEM)),
                scratch_shapes=[
                    pltpu.VMEM((n_dp, tokens, features), jnp.bfloat16),
                    pltpu.VMEM((n_dp, n_tp * rows, cols), jnp.bfloat16),
                    pltpu.VMEM((rows, model), jnp.bfloat16),
                    pltpu.VMEM((rows, model), jnp.bfloat16),
                    pltpu.VMEM((n_tp, lines, model // lines), jnp.float32),
                    pltpu.VMEM((n_dp, lines, model // lines), jnp.float32),
                    dma((4,)),
                    dma((n_dp, PIECES)), dma((n_dp, PIECES)),
                    dma((n_dp,)), dma((n_dp,)),
                    dma((n_z,)), dma((n_z,)), dma((n_z,)), dma((n_z,)),
                    dma((n_z,)), dma((n_z,)),
                    dma((n_tp,)), dma((n_tp,)), dma((n_dp,)), dma((n_dp,)),
                ],
                compiler_params=pltpu.CompilerParams(
                    collective_id=layer, has_side_effects=True, vmem_limit_bytes=60 * 1024 * 1024,
                ),
            )(proj_in[layer], kv_grad[layer], normed[layer], norm_grad[layer])
        new_first, new_second, update = adam_update(total / n_dp, first_moment[layer], second_moment[layer])
        firsts.append(new_first)
        seconds.append(new_second)
        updates.append(update)
        gains.append(gain.reshape(model))
    return (jnp.stack(firsts), jnp.stack(seconds), jnp.stack(updates), jnp.stack(gains))


def solution(mesh):
    return jax.shard_map(
        functools.partial(shards, mesh.shape["dp"], mesh.shape["tp"]),
        mesh=mesh,
        in_specs=(
            P(None, "dp", "tp"),
            P(None, ("dp", "tp"), None),
            P(None, ("dp", "tp"), None),
            P(None, ("dp", "tp"), None),
            P(None, "tp", "dp"),
            P(None, "tp", "dp"),
        ),
        out_specs=(P(None, "tp", "dp"), P(None, "tp", "dp"), P(None, "tp", "dp"), P()),
        check_vma=False,
    )
```

```python
import functools

import jax
import jax.numpy as jnp
from jax import lax
from jax.experimental import pallas as pl
from jax.experimental.pallas import tpu as pltpu
from jax.sharding import PartitionSpec as P

beta_one = 0.9
beta_two = 0.95
correct_one = 0.19
correct_two = 0.0975
epsilon = 1e-08
PIECES = 4
HEADS = 6


def adam_update(mean_grad, first_old, second_old):
    new_first = beta_one * first_old + (1.0 - beta_one) * mean_grad
    new_second = beta_two * second_old + (1.0 - beta_two) * mean_grad * mean_grad
    update = new_first / correct_one / (jnp.sqrt(new_second / correct_two) + epsilon)
    return (new_first, new_second, update)


def kernel(
    n_dp, n_tp, x_hbm, g_hbm, a_hbm, b_hbm, sum_ref, gain_ref,
    xs, kv, a_buf, b_buf, gain_tp, gain_dp,
    local_sem, x_send, x_recv, a2a_send, a2a_recv,
    up_send, up_recv, down_send, down_recv, pair_send, pair_recv,
    gt_send, gt_recv, gd_send, gd_recv,
):
    dp = lax.axis_index("dp")
    tp = lax.axis_index("tp")
    z = tp // 2
    core = tp % 2
    n_z = n_tp // 2
    rows = g_hbm.shape[0]
    cols = kv.shape[2]
    tokens = x_hbm.shape[0]
    piece = tokens // PIECES

    def dp_peer(o):
        return jnp.bitwise_xor(dp, o)

    def tp_peer(o):
        return lax.rem(tp + o, n_tp)

    locals_ = [
        pltpu.make_async_copy(a_hbm, a_buf, local_sem.at[0]),
        pltpu.make_async_copy(b_hbm, b_buf, local_sem.at[1]),
        pltpu.make_async_copy(
            g_hbm.at[:, pl.ds(pl.multiple_of(dp * cols, cols), cols)],
            kv.at[dp, pl.ds(pl.multiple_of(tp * rows, rows), rows), :],
            local_sem.at[2],
        ),
        pltpu.make_async_copy(x_hbm, xs.at[dp], local_sem.at[3]),
    ]
    for copy in locals_:
        copy.start()

    barrier = pltpu.get_barrier_semaphore()
    for o in range(1, n_dp):
        pl.semaphore_signal(barrier, inc=1, device_id={"dp": dp_peer(o)}, device_id_type=pl.DeviceIdType.MESH)
    for o in range(1, n_tp):
        pl.semaphore_signal(barrier, inc=1, device_id={"tp": tp_peer(o)}, device_id_type=pl.DeviceIdType.MESH)
    pl.semaphore_wait(barrier, n_dp - 1 + n_tp - 1)

    sent = []

    def remote(src, dst, send, recv, where):
        return pltpu.make_async_remote_copy(
            src_ref=src, dst_ref=dst, send_sem=send, recv_sem=recv,
            device_id=where, device_id_type=pl.DeviceIdType.MESH,
        )

    my_rows = pl.ds(pl.multiple_of(tp * rows, rows), rows)
    a2a = []
    for o in range(1, n_dp):
        peer = dp_peer(o)
        copy = remote(
            g_hbm.at[:, pl.ds(pl.multiple_of(peer * cols, cols), cols)],
            kv.at[dp, my_rows, :], a2a_send.at[o], a2a_recv.at[o], {"dp": peer},
        )
        copy.start()
        a2a.append(copy)
        sent.append(copy)

    def x_copy(src, origin, c, o_recv, o_to, send):
        part = pl.ds(c * piece, piece)
        return remote(
            src.at[part, :], xs.at[origin, part, :], send, x_recv.at[o_recv, c],
            {"dp": dp_peer(o_to)},
        )

    square = n_dp == 4
    orders = {o: list(range(PIECES)) for o in range(1, n_dp)}
    half = PIECES // 2
    if square:
        orders[2] = list(range(half, PIECES)) + list(range(half))
        orders[3] = []

    def send_own(i):
        for o in range(1, n_dp):
            if i < len(orders[o]):
                c = orders[o][i]
                copy = x_copy(x_hbm, dp, c, o, o, x_send.at[o, c])
                copy.start()
                sent.append(copy)

    def got(o, c):
        x_copy(xs.at[dp_peer(o)], dp_peer(o), c, o, o, x_send.at[o, c]).wait_recv()

    def forward(i):
        for o, o_to in ((1, 2), (2, 1)):
            c = orders[o][i]
            got(o, c)
            copy = x_copy(xs.at[dp_peer(o)], dp_peer(o), c, 3, o_to, x_send.at[3, c])
            copy.start()
            sent.append(copy)

    send_own(0)
    send_own(1)

    locals_[0].wait()
    locals_[1].wait()
    wide = gain_tp.shape[2]
    lines = gain_tp.shape[1]
    for j in range(lines):
        s = pl.ds(j * wide, wide)
        products = a_buf[:, s].astype(jnp.float32) * b_buf[:, s].astype(jnp.float32)
        gain_tp[tp, pl.ds(j, 1), :] = jnp.sum(products, axis=0, keepdims=True)
    tp_copies = []
    for o in range(1, n_tp):
        copy = remote(gain_tp.at[tp], gain_tp.at[tp], gt_send.at[o], gt_recv.at[o], {"tp": tp_peer(o)})
        copy.start()
        sent.append(copy)
        tp_copies.append(copy)

    def block(b, c):
        return kv.at[:, pl.ds(pl.multiple_of((2 * b + c) * rows, rows), rows), :]

    other = 2 * z + 1 - core

    def to_pair(b):
        return remote(block(b, core), block(b, core), pair_send.at[b], pair_recv.at[b], {"tp": other})

    def up(s):
        b = z - s + 1
        return remote(block(b, core), block(b, core), up_send.at[s], up_recv.at[s], {"tp": tp + 2})

    def down(s):
        b = z + s - 1
        return remote(block(b, core), block(b, core), down_send.at[s], down_recv.at[s], {"tp": tp - 2})

    def up_got(s):
        b = z - s
        return remote(block(b, core), block(b, core), up_send.at[s], up_recv.at[s], {"tp": other})

    def down_got(s):
        b = z + s
        return remote(block(b, core), block(b, core), down_send.at[s], down_recv.at[s], {"tp": other})

    locals_[2].wait()
    for o in range(1, n_dp):
        a2a[o - 1].wait_recv()

    for s in range(1, n_z + 1):
        if s > 1:
            @pl.when(z - s + 1 >= 0)
            def _():
                up_got(s - 1).wait_recv()

        if s < n_z:
            @pl.when((z - s + 1 >= 0) & (z + 1 < n_z))
            def _():
                up(s).start()

        if s > 1:
            @pl.when(z + s - 1 < n_z)
            def _():
                down_got(s - 1).wait_recv()

        if s < n_z:
            @pl.when((z + s - 1 < n_z) & (z - 1 >= 0))
            def _():
                down(s).start()

        if s == 1:
            to_pair(z).start()
        else:
            @pl.when(z - s + 1 >= 0)
            def _():
                to_pair(z - s + 1).start()

            @pl.when(z + s - 1 < n_z)
            def _():
                to_pair(z + s - 1).start()

        if s == 1:
            for copy in tp_copies:
                copy.wait_recv()
            gain_dp[dp, :, :] = jnp.sum(gain_tp[...], axis=0)
            for o in range(1, n_dp):
                copy = remote(gain_dp.at[dp], gain_dp.at[dp], gd_send.at[o], gd_recv.at[o], {"dp": dp_peer(o)})
                copy.start()
                sent.append(copy)
            for i in range(2, PIECES):
                send_own(i)
        if square and 2 <= s < 2 + half:
            forward(s - 2)
    if square:
        for i in range(max(n_z - 1, 0), half):
            forward(i)

    for b in range(n_z):
        remote(block(b, 1 - core), block(b, 1 - core), pair_send.at[b], pair_recv.at[b], {"tp": other}).wait_recv()

    width = min(256, sum_ref.shape[0])

    def multiply(origin, start, size, first=False):
        @pl.loop(0, sum_ref.shape[0] // width)
        def _(f):
            at = pl.ds(pl.multiple_of(f * width, width), width)
            part = lax.dot_general(
                xs[origin, pl.ds(start, size), at], kv[origin, pl.ds(start, size), :],
                (((0,), (0,)), ((), ())), preferred_element_type=jnp.float32,
            )
            if first:
                sum_ref[at, :] = part
            else:
                sum_ref[at, :] += part

    locals_[3].wait()
    multiply(dp, 0, tokens, True)
    for o in range(1, n_dp):
        if square and o == 3:
            continue
        for c in orders[o]:
            if not (square and c in orders[o][:half]):
                got(o, c)
        multiply(dp_peer(o), 0, tokens)

    for o in range(1, n_dp):
        remote(gain_dp.at[dp_peer(o)], gain_dp.at[dp_peer(o)], gd_send.at[o], gd_recv.at[o], {"dp": dp_peer(o)}).wait_recv()
    gain_ref[...] = jnp.sum(gain_dp[...], axis=0) / n_dp

    if square:
        for i in range(half):
            for o in (1, 2):
                c = orders[o][i]
                got(3, c)
                multiply(dp_peer(3), c * piece, piece)

    for copy in sent:
        copy.wait_send()
    for s in range(1, n_z):
        @pl.when((z - s + 1 >= 0) & (z + 1 < n_z))
        def _():
            up(s).wait_send()

        @pl.when((z + s - 1 < n_z) & (z - 1 >= 0))
        def _():
            down(s).wait_send()
    for b in range(n_z):
        to_pair(b).wait_send()


def square_kernel(
    n_tp, x_hbm, g_hbm, a_hbm, b_hbm, sum_ref, gain_ref,
    xs, xb, kv, kvp, part, arrived, a_buf, b_buf, gain_pair, gain_z, gain_dp,
    local_sem, head_send, head_recv, whole_send, whole_recv, fwd_send, fwd_recv,
    part_send, part_recv, a2a_send, a2a_recv,
    up_send, up_recv, down_send, down_recv, pair_send, pair_recv,
    gp_send, gp_recv, gz_send, gz_recv, gd_send, gd_recv,
):
    n_dp = 4
    dp = lax.axis_index("dp")
    tp = lax.axis_index("tp")
    z = tp // 2
    core = tp % 2
    n_z = n_tp // 2
    rows = g_hbm.shape[0]
    cols = kv.shape[2]
    tokens, features = x_hbm.shape
    head = part.shape[0]
    tail = features - head
    chunk = head // HEADS
    half = tokens // 2
    other = 2 * z + 1 - core
    sent = []

    def dp_peer(o):
        return jnp.bitwise_xor(dp, o)

    def remote(src, dst, send, recv, where):
        return pltpu.make_async_remote_copy(
            src_ref=src, dst_ref=dst, send_sem=send, recv_sem=recv,
            device_id=where, device_id_type=pl.DeviceIdType.MESH,
        )

    def go(copy):
        copy.start()
        sent.append(copy)

    my_rows = pl.ds(pl.multiple_of(tp * rows, rows), rows)

    def g_cols(d):
        return g_hbm.at[:, pl.ds(pl.multiple_of(d * cols, cols), cols)]

    locals_ = [
        pltpu.make_async_copy(g_cols(dp_peer(2)), kvp.at[0, my_rows, :], local_sem.at[0]),
        pltpu.make_async_copy(a_hbm, a_buf, local_sem.at[1]),
        pltpu.make_async_copy(b_hbm, b_buf, local_sem.at[2]),
        pltpu.make_async_copy(g_cols(dp), kv.at[dp, my_rows, :], local_sem.at[3]),
        pltpu.make_async_copy(x_hbm, xs.at[0], local_sem.at[4]),
    ]
    for copy in locals_:
        copy.start()

    barrier = pltpu.get_barrier_semaphore()
    for o in range(1, n_dp):
        pl.semaphore_signal(barrier, inc=1, device_id={"dp": dp_peer(o)}, device_id_type=pl.DeviceIdType.MESH)
    for o in range(1, n_tp):
        pl.semaphore_signal(barrier, inc=1, device_id={"tp": lax.rem(tp + o, n_tp)}, device_id_type=pl.DeviceIdType.MESH)
    pl.semaphore_wait(barrier, n_dp - 1 + n_tp - 1)

    pair_base = dp // 2 * 2
    groups = [
        kvp.at[pl.ds(0, 1)],
        kvp.at[pl.ds(1, 1)],
        kv.at[pl.ds(pair_base, 2)],
        kv.at[pl.ds(2 - pair_base, 2)],
    ]

    def block(g, b, c):
        return groups[g].at[:, pl.ds(pl.multiple_of((2 * b + c) * rows, rows), rows), :]

    def to_pair(g, b):
        return remote(block(g, b, core), block(g, b, core), pair_send.at[g, b], pair_recv.at[g, b], {"tp": other})

    def from_pair(g, b):
        return remote(block(g, b, 1 - core), block(g, b, 1 - core), pair_send.at[g, b], pair_recv.at[g, b], {"tp": other})

    def up(g, s):
        b = z - s + 1
        return remote(block(g, b, core), block(g, b, core), up_send.at[g, s], up_recv.at[g, s], {"tp": tp + 2})

    def down(g, s):
        b = z + s - 1
        return remote(block(g, b, core), block(g, b, core), down_send.at[g, s], down_recv.at[g, s], {"tp": tp - 2})

    def up_got(g, s):
        b = z - s
        return remote(block(g, b, core), block(g, b, core), up_send.at[g, s], up_recv.at[g, s], {"tp": other})

    def down_got(g, s):
        b = z + s
        return remote(block(g, b, core), block(g, b, core), down_send.at[g, s], down_recv.at[g, s], {"tp": other})

    def chain(g, s):
        if s > 1:
            @pl.when(z - s + 1 >= 0)
            def _():
                up_got(g, s - 1).wait_recv()

        if s < n_z:
            @pl.when((z - s + 1 >= 0) & (z + 1 < n_z))
            def _():
                up(g, s).start()

        if s > 1:
            @pl.when(z + s - 1 < n_z)
            def _():
                down_got(g, s - 1).wait_recv()

        if s < n_z:
            @pl.when((z + s - 1 < n_z) & (z - 1 >= 0))
            def _():
                down(g, s).start()

        if s == 1:
            to_pair(g, z).start()
        else:
            @pl.when(z - s + 1 >= 0)
            def _():
                to_pair(g, z - s + 1).start()

            @pl.when(z + s - 1 < n_z)
            def _():
                to_pair(g, z + s - 1).start()

    def complete(g):
        for b in range(n_z):
            from_pair(g, b).wait_recv()

    swap = remote(g_cols(dp_peer(3)), kvp.at[1, my_rows, :], a2a_send.at[0], a2a_recv.at[0], {"dp": dp_peer(1)})
    go(swap)
    locals_[0].wait()
    chain(0, 1)

    def a2a(o, origin):
        return remote(g_cols(dp_peer(o)), kv.at[origin, my_rows, :], a2a_send.at[o], a2a_recv.at[o], {"dp": dp_peer(o)})

    for o in range(1, n_dp):
        go(a2a(o, dp))

    tail_at = pl.ds(head, tail)

    def head_copy(k):
        at = pl.ds(k * chunk, chunk)
        return remote(x_hbm.at[:, at], xs.at[1, :, at], head_send.at[k], head_recv.at[k], {"dp": dp_peer(1)})

    def tail_copy(o, h):
        at = pl.ds(h * half, half)
        dst = xs.at[1, at, tail_at] if o == 1 else xb.at[0, at, :]
        return remote(x_hbm.at[at, tail_at], dst, whole_send.at[o, h], whole_recv.at[o, h], {"dp": dp_peer(o)})

    def forward(h):
        at = pl.ds(h * half, half)
        src = xs.at[1, at, tail_at] if h == 0 else xb.at[0, at, :]
        return remote(src, xb.at[1, at, :], fwd_send.at[h], fwd_recv.at[h], {"dp": dp_peer(2 - h)})

    early = HEADS // 2
    for k in range(early):
        go(head_copy(k))
    go(tail_copy(2, 1))
    go(tail_copy(2, 0))

    locals_[1].wait()
    locals_[2].wait()
    wide = gain_pair.shape[2]

    def gain_lines(lo, hi):
        for j in range(lo, hi):
            at = pl.ds(j * wide, wide)
            products = a_buf[:, at].astype(jnp.float32) * b_buf[:, at].astype(jnp.float32)
            gain_pair[core, pl.ds(j, 1), :] = jnp.sum(products, axis=0, keepdims=True)

    lines = gain_pair.shape[1]
    gain_lines(0, lines)
    swap.wait_recv()
    chain(1, 1)
    gain_core = remote(gain_pair.at[core], gain_pair.at[core], gp_send.at[0], gp_recv.at[0], {"tp": other})
    go(gain_core)
    for s in range(2, n_z + 1):
        chain(0, s)
        chain(1, s)

    gain_core.wait_recv()
    gain_z[z, :, :] = jnp.sum(gain_pair[...], axis=0)
    for o in range(1, n_z):
        go(remote(gain_z.at[z], gain_z.at[z], gz_send.at[o], gz_recv.at[o], {"tp": lax.rem(tp + 2 * o, n_tp)}))

    for o in (1, 2, 3):
        a2a(o, dp_peer(o)).wait_recv()
    locals_[3].wait()
    chain(2, 1)
    locals_[4].wait()
    for k in range(early, HEADS):
        go(head_copy(k))
    complete(0)
    complete(1)

    def dot(x, w):
        return lax.dot_general(x, w, (((0,), (0,)), ((), ())), preferred_element_type=jnp.float32)

    def part_copy(k):
        at = pl.ds(k * chunk, chunk)
        return remote(part.at[at, :], arrived.at[at, :], part_send.at[k], part_recv.at[k], {"dp": dp_peer(2)})

    for k in range(HEADS):
        at = pl.ds(k * chunk, chunk)
        head_copy(k).wait_recv()
        part[at, :] = dot(xs[0, :, at], kvp[0]) + dot(xs[1, :, at], kvp[1])
        go(part_copy(k))
        if k == 1:
            for o in range(1, n_z):
                copy = remote(
                    gain_z.at[lax.rem(z + o, n_z)], gain_z.at[lax.rem(z + o, n_z)],
                    gz_send.at[n_z - o], gz_recv.at[n_z - o], {"tp": other},
                )
                copy.wait_recv()
            gain_dp[dp, :, :] = jnp.sum(gain_z[...], axis=0)
            for o in range(1, n_dp):
                go(remote(gain_dp.at[dp], gain_dp.at[dp], gd_send.at[o], gd_recv.at[o], {"dp": dp_peer(o)}))
            chain(2, 2)
        if k == 2:
            go(tail_copy(1, 0))
            go(tail_copy(1, 1))
        if k == 3:
            tail_copy(2, 1).wait_recv()
            go(forward(1))
            chain(2, 3)
            chain(3, 1)
        if k == HEADS - 2:
            for s in range(4, n_z + 1):
                chain(2, s)
    complete(2)
    chain(3, 2)

    def head_sum(k):
        at = pl.ds(k * chunk, chunk)
        sum_ref[at, :] = dot(xs[0, :, at], kv[dp]) + dot(xs[1, :, at], kv[dp_peer(1)])

    for k in range(HEADS // 2):
        head_sum(k)
    tail_copy(1, 0).wait_recv()
    go(forward(0))
    chain(3, 3)
    for k in range(HEADS // 2, HEADS):
        head_sum(k)
    tail_copy(1, 1).wait_recv()
    sum_ref[tail_at, :] = dot(xs[0, :, tail_at], kv[dp]) + dot(xs[1, :, tail_at], kv[dp_peer(1)])
    for s in range(4, n_z + 1):
        chain(3, s)
    for o in range(1, n_dp):
        remote(gain_dp.at[dp_peer(o)], gain_dp.at[dp_peer(o)], gd_send.at[o], gd_recv.at[o], {"dp": dp_peer(o)}).wait_recv()
    total_gain = jnp.sum(gain_dp[...], axis=0) / n_dp
    for i in range(wide // 128):
        gain_ref[pl.ds(i, lines, stride=wide // 128), :] = total_gain[:, i * 128:(i + 1) * 128]
    for k in range(HEADS):
        at = pl.ds(k * chunk, chunk)
        part_copy(k).wait_recv()
        sum_ref[at, :] += arrived[at, :]
    complete(3)
    tail_copy(2, 0).wait_recv()
    sum_ref[tail_at, :] += dot(xb[0], kv[dp_peer(2)])
    for h in (1, 0):
        forward(h).wait_recv()
        at = pl.ds(h * half, half)
        sum_ref[tail_at, :] += dot(xb[1, at, :], kv[dp_peer(3), at, :])

    for copy in sent:
        copy.wait_send()
    for g in range(len(groups)):
        for s in range(1, n_z):
            @pl.when((z - s + 1 >= 0) & (z + 1 < n_z))
            def _():
                up(g, s).wait_send()

            @pl.when((z + s - 1 < n_z) & (z - 1 >= 0))
            def _():
                down(g, s).wait_send()
        for b in range(n_z):
            to_pair(g, b).wait_send()


def square_call(layer, n_tp, x, g, a, b):
    tokens, features = x.shape
    rows, width = g.shape
    model = a.shape[1]
    n_dp = 4
    cols = width // n_dp
    lines = 8
    n_z = n_tp // 2
    head = features // (HEADS + 2) * HEADS
    dma = pltpu.SemaphoreType.DMA
    bf16, f32 = jnp.bfloat16, jnp.float32
    buffers = [
        ((2, tokens, features), bf16), ((2, tokens, features - head), bf16),
        ((n_dp, tokens, cols), bf16), ((2, tokens, cols), bf16),
        ((head, cols), f32), ((head, cols), f32),
        ((rows, model), bf16), ((rows, model), bf16),
        ((2, lines, model // lines), f32), ((n_z, lines, model // lines), f32), ((n_dp, lines, model // lines), f32),
    ]
    return pl.pallas_call(
        functools.partial(square_kernel, n_tp),
        out_shape=(
            jax.ShapeDtypeStruct((features, cols), f32),
            jax.ShapeDtypeStruct((model // 128, 128), f32),
        ),
        in_specs=[pl.BlockSpec(memory_space=pltpu.HBM)] * 4,
        out_specs=(pl.BlockSpec(memory_space=pltpu.VMEM), pl.BlockSpec(memory_space=pltpu.VMEM)),
        scratch_shapes=[pltpu.VMEM(shape, dtype) for shape, dtype in buffers] + [
            dma((5,)), dma((HEADS,)), dma((HEADS,)), dma((3, 2)), dma((3, 2)), dma((2,)), dma((2,)),
            dma((HEADS,)), dma((HEADS,)), dma((n_dp,)), dma((n_dp,)),
        ] + [dma((4, n_z))] * 6 + [
            dma((1,)), dma((1,)), dma((n_z,)), dma((n_z,)), dma((n_dp,)), dma((n_dp,)),
        ],
        compiler_params=pltpu.CompilerParams(
            collective_id=layer, has_side_effects=True, vmem_limit_bytes=50 * 1024 * 1024,
        ),
    )(x, g, a, b)


def shards(n_dp, n_tp, proj_in, kv_grad, normed, norm_grad, first_moment, second_moment):
    layers, tokens, features = proj_in.shape
    rows, width = kv_grad.shape[1:]
    model = normed.shape[2]
    cols = width // n_dp
    lines = 8
    dma = pltpu.SemaphoreType.DMA
    n_z = n_tp // 2
    firsts, seconds, updates, gains = [], [], [], []
    for layer in range(layers):
        if n_dp == 4 and features % (128 * (HEADS + 2)) == 0 and n_tp >= 6:
            total, gain = square_call(layer, n_tp, proj_in[layer], kv_grad[layer], normed[layer], norm_grad[layer])
        else:
            total, gain = pl.pallas_call(
                functools.partial(kernel, n_dp, n_tp),
                out_shape=(
                    jax.ShapeDtypeStruct((features, cols), jnp.float32),
                    jax.ShapeDtypeStruct((lines, model // lines), jnp.float32),
                ),
                in_specs=[pl.BlockSpec(memory_space=pltpu.HBM)] * 4,
                out_specs=(pl.BlockSpec(memory_space=pltpu.VMEM), pl.BlockSpec(memory_space=pltpu.VMEM)),
                scratch_shapes=[
                    pltpu.VMEM((n_dp, tokens, features), jnp.bfloat16),
                    pltpu.VMEM((n_dp, n_tp * rows, cols), jnp.bfloat16),
                    pltpu.VMEM((rows, model), jnp.bfloat16),
                    pltpu.VMEM((rows, model), jnp.bfloat16),
                    pltpu.VMEM((n_tp, lines, model // lines), jnp.float32),
                    pltpu.VMEM((n_dp, lines, model // lines), jnp.float32),
                    dma((4,)),
                    dma((n_dp, PIECES)), dma((n_dp, PIECES)),
                    dma((n_dp,)), dma((n_dp,)),
                    dma((n_z,)), dma((n_z,)), dma((n_z,)), dma((n_z,)),
                    dma((n_z,)), dma((n_z,)),
                    dma((n_tp,)), dma((n_tp,)), dma((n_dp,)), dma((n_dp,)),
                ],
                compiler_params=pltpu.CompilerParams(
                    collective_id=layer, has_side_effects=True, vmem_limit_bytes=60 * 1024 * 1024,
                ),
            )(proj_in[layer], kv_grad[layer], normed[layer], norm_grad[layer])
        new_first, new_second, update = adam_update(total / n_dp, first_moment[layer], second_moment[layer])
        firsts.append(new_first)
        seconds.append(new_second)
        updates.append(update)
        gains.append(gain.reshape(model))
    return (jnp.stack(firsts), jnp.stack(seconds), jnp.stack(updates), jnp.stack(gains))


def solution(mesh):
    return jax.shard_map(
        functools.partial(shards, mesh.shape["dp"], mesh.shape["tp"]),
        mesh=mesh,
        in_specs=(
            P(None, "dp", "tp"),
            P(None, ("dp", "tp"), None),
            P(None, ("dp", "tp"), None),
            P(None, ("dp", "tp"), None),
            P(None, "tp", "dp"),
            P(None, "tp", "dp"),
        ),
        out_specs=(P(None, "tp", "dp"), P(None, "tp", "dp"), P(None, "tp", "dp"), P()),
        check_vma=False,
    )
```
